32 devices in a mesh: dp: 8 (over y, x, core), tensor: 4 (over z).
Axes of the slice: x: 2, y: 2, z: 4, core: 2. Of those that a mesh axis runs over, the one named last changes fastest.
Arguments:
- acts: bfloat16 [8192, 3584], P('dp'), may hold values from -6 to 6
- cotangent: bfloat16 [8192, 18944], P('dp', 'tensor'), may hold values from -6 to 6
- hessian_ema: float32 [3584, 18944], P('dp', 'tensor'), may hold values from 0.02 to 2
- momentum: float32 [3584, 18944], P('dp', 'tensor'), may hold values from -0.12 to 0.12
- gamma_table: float32 [28], replicated, may hold values from 0.005 to 0.02
- layer_index: int32 [1], replicated, may hold values from 0 to 27
- step_count: int32 [1], replicated, may hold values from 1 to 20
Outputs:
- new_hessian: float32 [67895296], P(('dp', 'tensor'))
- ratio: float32 [67895296], P(('dp', 'tensor'))
The draws below stay inside these ranges and needn't reach their ends.
All inputs are finite; a program needn't handle non-finite values.
Results may differ from the reference program's by a relative error of at most 0.0003.
Values sent between devices are 32-bit elements; how exact they have to be, the bound alone decides.
No kernel may reach another device: no remote copies, remote signals or barrier semaphores. Data moves between devices by JAX's collectives and lax.ppermute only.
A program may use at most 192 MiB of HBM per device.

```python
import math
import jax
import jax.numpy as jnp
from jax import lax

D = 3584
FF = 18944
LAYERS_ALL = 28
TOKENS = 8192


def raised(array, rng, source, target, parts, factor):
    def block_of(axis_at):
        return (jnp.arange(array.shape[axis_at]) // (array.shape[axis_at] // parts)).reshape((-1,) + (1,) * (array.ndim - 1 - axis_at))

    one_side = jax.random.permutation(rng, parts)[block_of(target)]
    far = (block_of(target) + parts // 2) % parts
    return jnp.where((block_of(source) == one_side) | (block_of(source) == far), factor * array, array)


def block_scale(rng, shape, pieces, least, top_value):
    loudness = 1.0
    for axis_at, shards_of in pieces:
        draws = jax.random.uniform(jax.random.fold_in(jax.random.fold_in(rng, 6), axis_at), (shards_of,), jnp.float32, least / len(pieces), top_value / len(pieces))
        loudness = loudness * jnp.repeat(jnp.exp(draws), shape[axis_at] // shards_of).reshape((-1,) + (1,) * (len(shape) - 1 - axis_at))
    return loudness


def normal_values(own_key, dims, deviation, limit, shards=(), kind=jnp.bfloat16):
    array = deviation * jax.random.normal(own_key, dims, jnp.float32)
    if shards:
        array = array * block_scale(own_key, dims, shards, -0.22, 0.18)
    return jnp.clip(array, -limit, limit).astype(kind)


def gaussian_with(stream_key, extent, spread, reach, pieces, heavy, kind=jnp.bfloat16):
    values = spread * jax.random.normal(stream_key, extent, jnp.float32)
    if pieces:
        values = values * block_scale(stream_key, extent, pieces, -0.22, 0.18)
    return jnp.clip(raised(values, jax.random.fold_in(stream_key, 3), *heavy), -reach, reach).astype(kind)


def setup_inputs(seed: int = 0) -> dict:
    key_list = jax.random.split(jax.random.key(seed), 8)
    acts = gaussian_with(key_list[0], (TOKENS, D), 1.0, 6.0, ((0, 8),), (0, 1, 8, 2.0))
    cotangent = normal_values(key_list[1], (TOKENS, FF), 1.0, 6.0, ((0, 8), (1, 4)))
    hessian_ema = jnp.clip(jnp.exp(math.log(2.0) - 4.6051702 * jax.random.uniform(key_list[2], (D, FF), jnp.float32) ** block_scale(key_list[2], (D, FF), ((0, 8), (1, 4)), -0.2, 0.2)), 0.02, 2.0)
    momentum = normal_values(key_list[3], (D, FF), 0.02, 0.12, ((0, 8), (1, 4)), jnp.float32)
    gamma_table = jnp.clip(jnp.exp(jax.random.uniform(key_list[4], (LAYERS_ALL,), jnp.float32, math.log(0.005), math.log(0.02))), 0.005, 0.02)
    layer_index = jax.random.randint(key_list[5], (1,), 0, LAYERS_ALL).astype(jnp.int32)
    step_count = jax.random.randint(key_list[6], (1,), 1, 21).astype(jnp.int32)
    return {"acts": acts, "cotangent": cotangent, "hessian_ema": hessian_ema, "momentum": momentum, "gamma_table": gamma_table, "layer_index": layer_index, "step_count": step_count}


def reference(acts, cotangent, hessian_ema, momentum, gamma_table, layer_index, step_count):
    grad_sum = lax.dot_general(acts, cotangent, (((0,), (0,)), ((), ())), preferred_element_type=jnp.float32)
    estimate = grad_sum * grad_sum / float(TOKENS)
    fresh = 0.99 * hessian_ema + 0.01 * estimate
    picks = jnp.arange(LAYERS_ALL, dtype=jnp.int32) == layer_index[0]
    gamma = jnp.sum(jnp.where(picks, gamma_table, jnp.zeros_like(gamma_table)))
    correction = 1.0 - jnp.power(jnp.asarray(0.99, gamma_table.dtype), step_count[0].astype(gamma_table.dtype))
    corrected = fresh / correction
    ratio = jnp.clip(momentum / (gamma * corrected), -1.0, 1.0)
    return fresh.reshape(-1), ratio.reshape(-1)
```

```python
import jax
import jax.numpy as jnp
from jax import lax
from jax.experimental import pallas as pl
from jax.experimental.pallas import tpu as pltpu
from jax.sharding import PartitionSpec as P

LANES = 128
SUBLANES = 8
WRITE_LAG = 2


def row_chunks(rows):
    step = 16
    if rows % step:
        return [rows]
    count = rows // step
    double = count // 3
    return [2 * step] * double + [step] * (count - 2 * double)


def flat_kernel(where, scal, *refs, tp, per_row):
    fresh_in = refs[:tp]
    mom_in = refs[tp : 2 * tp]
    fresh_out, ratio_out = refs[-2:]
    gamma = scal[0]
    correction = scal[1]
    for s in range(tp):
        base = where[s] * per_row
        for j in range(per_row):
            cols = slice(j * LANES, (j + 1) * LANES)
            fresh = fresh_in[s][:, cols]
            ratio = jnp.clip(mom_in[s][:, cols] / (gamma * (fresh / correction)), -1.0, 1.0)
            rows = pl.ds(base + j, SUBLANES, stride=tp * per_row)
            fresh_out[rows, :] = fresh
            ratio_out[rows, :] = ratio


def write_flat(where, scal, fresh, mom, first, rows, outs):
    tp = len(fresh)
    n, cols = fresh[0].shape
    per_row = cols // LANES
    step0 = first // SUBLANES
    own_step = rows // SUBLANES
    in_specs = [pl.BlockSpec((SUBLANES, cols), lambda i, *_: (i, 0)) for _ in range(tp)]
    in_specs.append(pl.BlockSpec((SUBLANES, cols), lambda i, where, scal: (where[0] * own_step + step0 + i, 0)))
    in_specs += [pl.BlockSpec((SUBLANES, cols), lambda i, *_: (step0 + i, 0)) for _ in range(tp - 1)]
    block = (SUBLANES * tp * per_row, LANES)
    out_specs = [pl.BlockSpec(block, lambda i, *_: (step0 + i, 0)) for _ in range(2)]
    shape = jax.ShapeDtypeStruct((rows * tp * per_row, LANES), jnp.float32)
    aliases = {}
    if outs is not None:
        in_specs += [pl.BlockSpec(memory_space=pl.ANY)] * 2
        aliases = {2 + 2 * tp: 0, 3 + 2 * tp: 1}

    def body(where, scal, *refs):
        flat_kernel(where, scal, *refs, tp=tp, per_row=per_row)

    return pl.pallas_call(
        body,
        grid_spec=pltpu.PrefetchScalarGridSpec(
            num_scalar_prefetch=2,
            grid=(n // SUBLANES,),
            in_specs=in_specs,
            out_specs=out_specs,
        ),
        out_shape=(shape, shape),
        input_output_aliases=aliases,
        compiler_params=pltpu.CompilerParams(dimension_semantics=("arbitrary",)),
        name="write_flat",
    )(where, scal, *fresh, *mom, *(outs or ()))


def turn_kernel(where, acts_ref, *refs, chunks, dp, tp, rows):
    outs, scratch = refs[:-1], refs[-1]
    step = pl.program_id(0)
    width = acts_ref.shape[1]
    scratch[pl.ds(pl.multiple_of(step * width, width), width), :] = acts_ref[...].T

    @pl.when(step == pl.num_programs(0) - 1)
    def _():
        first = 0
        for k, n in enumerate(chunks):
            for core in range(2):
                for delta in range(dp // 2):
                    for s in range(tp):
                        row = where[(2 * delta + 1 - core) * tp + s] * rows + first
                        at = (delta * tp + s) * n
                        outs[2 * k + core][at : at + n, :] = scratch[pl.ds(pl.multiple_of(row, 16), n), :]
            first += n


def acts_by_chunk(acts, me, at, dp, tp, chunks):
    tokens, width = acts.shape
    rows = width // (dp * tp)
    deltas = me ^ jnp.arange(dp, dtype=jnp.int32)
    turns = (at + jnp.arange(tp, dtype=jnp.int32)) % tp
    order = (deltas[:, None] * tp + turns[None, :]).reshape(-1)
    wide = 512
    if rows % 16 or width % wide:
        whole = jnp.take(acts.T.reshape(dp * tp, rows, tokens), order, axis=0, mode="clip")
        whole = whole.reshape(dp // 2, 2, tp, rows, tokens)
        out, first = [], 0
        for n in chunks:
            for core in (1, 0):
                out.append(whole[:, core, :, first : first + n].reshape(-1, tokens))
            first += n
        return out

    def body(where, acts_ref, *refs):
        turn_kernel(where, acts_ref, *refs, chunks=chunks, dp=dp, tp=tp, rows=rows)

    shapes = [jax.ShapeDtypeStruct((dp // 2 * tp * n, tokens), acts.dtype) for n in chunks for _ in range(2)]
    return pl.pallas_call(
        body,
        grid_spec=pltpu.PrefetchScalarGridSpec(
            num_scalar_prefetch=1,
            grid=(width // wide,),
            in_specs=[pl.BlockSpec((tokens, wide), lambda i, *_: (0, i))],
            out_specs=[pl.BlockSpec(s.shape, lambda i, *_: (0, 0)) for s in shapes],
            scratch_shapes=[pltpu.VMEM((width, tokens), acts.dtype)],
        ),
        out_shape=shapes,
        compiler_params=pltpu.CompilerParams(dimension_semantics=("arbitrary",), vmem_limit_bytes=48 * 1024 * 1024),
        name="acts_turn",
    )(order, acts)


def after(x, dep):
    return lax.optimization_barrier((x, dep))[0]


def product(lhs, rhs):
    return lax.dot_general(lhs, rhs, (((1,), (0,)), ((), ())), preferred_element_type=jnp.float32)


def on_device(acts, cotangent, hessian_ema, momentum, gamma_table, layer_index, step_count, dp, tp):
    tokens, width = acts.shape
    cols = cotangent.shape[1]
    tokens_all = float(tokens * dp)
    rows = width // (dp * tp)
    picks = jnp.arange(gamma_table.shape[0], dtype=jnp.int32) == layer_index[0]
    gamma = jnp.sum(jnp.where(picks, gamma_table, jnp.zeros_like(gamma_table)))
    correction = 1.0 - jnp.power(
        jnp.asarray(0.99, gamma_table.dtype), step_count[0].astype(gamma_table.dtype)
    )
    me = lax.axis_index("dp")
    at = lax.axis_index("tensor")
    bits = dp.bit_length() - 1

    def turn(x, s):
        return lax.ppermute(x, "tensor", [(i, (i + s) % tp) for i in range(tp)])

    def swap(x, b):
        return lax.ppermute(x, "dp", [(i, i ^ (1 << b)) for i in range(dp)])

    hess = hessian_ema.reshape(tp, rows, cols)
    mom = momentum.reshape(tp, rows, cols)

    def block(x, s):
        return lax.dynamic_index_in_dim(x, (at + s) % tp, 0, keepdims=False)

    mom_moved, source = [], mom
    for s in range(1, tp):
        sent = block(source, s)
        mom_moved.append(turn(sent, s))
        source = after(mom, sent)

    chunks = row_chunks(rows)
    lhs = acts_by_chunk(acts, me, at, dp, tp, chunks)

    where = (at - jnp.arange(tp, dtype=jnp.int32)) % tp
    scal = jnp.stack([gamma, correction])
    aligned = cols % LANES == 0 and rows % SUBLANES == 0
    halves = 2 if tp % 2 == 0 else 1
    firsts = [sum(chunks[:k]) for k in range(len(chunks))]
    stages = max(bits - 1, 1)

    def send_dot(k, dep):
        part = product(after(lhs[2 * k], dep), cotangent)
        return part, swap(part, 0)

    def own_dot(k, moved, dep):
        chip = product(after(lhs[2 * k + 1], dep), cotangent) + moved
        blocks = chip.reshape((2,) * (bits - 1) + (tp, chunks[k], cols))
        parts = []
        for h in range(halves):
            axes = list(range(1, bits))
            if h:
                axes.reverse()
            half = blocks[..., h * tp // halves : (h + 1) * tp // halves, :, :]
            parts.append(([half], axes, list(range(bits - 1, 0, -1))))
        return chip, parts

    def exchange(parts, stage, dep):
        out = []
        for terms, axes, left in parts:
            b = axes[stage]
            pos = left.index(b)
            sides = [lax.index_in_dim(x, 1, pos, keepdims=False) for x in terms]
            sides[0] = after(sides[0], dep)
            send = sum(sides[1:], sides[0])
            dep = send
            moved = swap(send, b)
            keep = [lax.index_in_dim(x, 0, pos, keepdims=False) for x in terms]
            out.append((keep + [moved], axes, [x for x in left if x != b]))
        return out, dep

    def fresh_of(k, parts, dep):
        own = slice(firsts[k], firsts[k] + chunks[k])
        source = after(hess, dep)
        out = []
        for s in range(tp):
            terms = [x[s % (tp // halves)] for x in parts[s * halves // tp][0]]
            grad = sum(terms[1:], terms[0])
            estimate = grad * grad / tokens_all
            out.append(0.99 * block(source[:, own], s) + 0.01 * estimate)
        moved = [out[0]]
        for s in range(1, tp):
            moved.append(turn(out[s], s))
        return moved, out[-1]

    def write(k, outs, dep):
        return write_flat(where, after(scal, dep), fresh[k], [momentum, *mom_moved], firsts[k], rows, outs)

    count = len(chunks)
    pairs, parts, fresh, outs = {}, {}, {}, None
    dep = lhs[0]
    for k in range(min(2, count)):
        dep, pairs[k] = send_dot(k, dep)
    for step in range(count + stages):
        if step < count:
            dep, parts[step] = own_dot(step, pairs[step], dep)
        for stage in range(stages):
            j = step - stage
            if 0 <= j < count:
                parts[j], dep = exchange(parts[j], stage, dep)
        j = step - stages
        if 0 <= j < count:
            if aligned and j >= WRITE_LAG:
                outs = write(j - WRITE_LAG, outs, dep)
                dep = outs[0]
            fresh[j], dep = fresh_of(j, parts[j], dep)
        if step + 2 < count:
            dep, pairs[step + 2] = send_dot(step + 2, dep)
    if aligned:
        for j in range(max(count - WRITE_LAG, 0), count):
            outs = write(j, outs, dep)
    pieces = [fresh[k] for k in range(count)]
    if aligned:
        return tuple(o.reshape(-1) for o in outs)
    fresh = [jnp.concatenate([p[s] for p in pieces], axis=0) for s in range(tp)]
    moms = [block(mom, 0), *mom_moved]

    def in_order(parts):
        stacked = jnp.stack(parts)
        return jnp.concatenate([lax.dynamic_index_in_dim(stacked, (at - i) % tp, 0, keepdims=False) for i in range(tp)], axis=1)

    fresh_rows = in_order(fresh)
    ratio = jnp.clip(in_order(moms) / (gamma * (fresh_rows / correction)), -1.0, 1.0)
    return fresh_rows.reshape(-1), ratio.reshape(-1)


def solution(mesh):
    dp, tp = mesh.shape["dp"], mesh.shape["tensor"]
    placed = (P("dp", None), P("dp", "tensor"), P("dp", "tensor"), P("dp", "tensor"), P(), P(), P())

    def body(*args):
        return on_device(*args, dp=dp, tp=tp)

    return jax.shard_map(
        body,
        mesh=mesh,
        in_specs=placed,
        out_specs=(P(("dp", "tensor")), P(("dp", "tensor"))),
        check_vma=False,
    )
```
